512 devices in a mesh: facet: 64 (over y, z_hi, x), band: 4 (over z_lo), sub: 2 (over core).
Axes of the slice: x: 4, y: 4, z: 16 (z_hi: 4, z_lo: 4; z = z_hi * 4 + z_lo), core: 2. Of those that a mesh axis runs over, the one named last changes fastest.
Arguments:
- facets: bfloat16 [131072, 2048], P(('facet', 'band')), may hold values from -6 to 6
- window: float32 [2048], replicated, may hold values from 0.5 to 1.5
- facet_offsets: int32 [64, 2], replicated, may hold values from 0 to 49151
- row_offsets: int32 [8], replicated, may hold values from 0 to 49151
- column_offset: int32 [1], replicated, may hold values from 0 to 49151
- kernel: bfloat16 [256, 256], replicated, may hold values from -0.375 to 0.375
- tile_counts: int32 [8, 16, 16], replicated, may hold values from 0 to 32
Outputs:
- residual: bfloat16 [131072, 2048], P(('facet', 'band'))
The draws below stay inside these ranges and needn't reach their ends.
All inputs are finite; a program needn't handle non-finite values.
Results may differ from the reference program's by a relative error of at most 0.013.
Values may be sent and summed in bfloat16 or wider, within the bound.
No kernel may reach another device: no remote copies, remote signals or barrier semaphores. Data moves between devices by JAX's collectives and lax.ppermute only.
A program may use at most 64 MiB of HBM per device.

```python
import math
import jax
import jax.numpy as jnp
from jax import lax

IMAGE = 49152
FACET = 2048
CONTRIB = 256
TILE = 16
FACETS = 64
SUBGRIDS = 8


def with_ends(array, stream_key, least, largest):
    extent = array.shape
    spot = [jax.random.randint(jax.random.fold_in(stream_key, axis), (), 0, extent[axis]) for axis in range(len(extent))]
    array = array.at[tuple(spot)].set(least)
    longest = extent.index(max(extent))
    spot[longest] = (spot[longest] + 1) % extent[longest]
    return array.at[tuple(spot)].set(largest)


def levels(key, dims, shards, least, top_value):
    loudness = 1.0
    for dim, parts in shards:
        draws = jax.random.uniform(jax.random.fold_in(jax.random.fold_in(key, 6), dim), (parts,), jnp.float32, least / len(shards), top_value / len(shards))
        loudness = loudness * jnp.repeat(jnp.exp(draws), dims[dim] // parts).reshape((-1,) + (1,) * (len(dims) - 1 - dim))
    return loudness


def scatter_about(rng, shape, scale, reach, cuts=(), held_as=jnp.bfloat16):
    array = jax.random.normal(rng, shape, jnp.float32) * scale
    if len(cuts) > 0:
        array = levels(rng, shape, cuts, -0.22, 0.18) * array
    return jnp.clip(array, min=-reach, max=reach).astype(held_as)


def setup_inputs(seed: int = 0) -> dict:
    splits = jax.random.split(jax.random.key(seed), 8)
    facets = scatter_about(splits[0], (FACETS * FACET, FACET), 1.0, 6.0, ((0, 256),))
    window = jnp.clip(jax.random.uniform(splits[1], (FACET,), jnp.float32, 0.5, 1.5), 0.5, 1.5)
    facet_offsets = with_ends(jax.random.randint(splits[2], (FACETS, 2), 0, IMAGE), jax.random.fold_in(splits[2], 1), 0, IMAGE - 1).astype(jnp.int32)
    row_offsets = with_ends(jax.random.randint(splits[3], (SUBGRIDS,), 0, IMAGE), jax.random.fold_in(splits[3], 1), 0, IMAGE - 1).astype(jnp.int32)
    column_offset = jax.random.randint(splits[4], (1,), 0, IMAGE).astype(jnp.int32)
    kernel = scatter_about(splits[5], (CONTRIB, CONTRIB), CONTRIB ** -0.5, 0.375)
    tile_counts = with_ends(jax.random.randint(splits[6], (SUBGRIDS, CONTRIB // TILE, CONTRIB // TILE), 0, 33), jax.random.fold_in(splits[6], 1), 0, 32).astype(jnp.int32)
    return {"facets": facets, "window": window, "facet_offsets": facet_offsets, "row_offsets": row_offsets, "column_offset": column_offset, "kernel": kernel, "tile_counts": tile_counts}


def modular_product(first, second):
    upper_bits = first // 256
    lower_bits = first % 256
    reduced = upper_bits * second % IMAGE
    reduced = reduced * 256 % IMAGE
    return (reduced + lower_bits * second) % IMAGE

def phase_table(frequency, position):
    reduced = modular_product(frequency % IMAGE, position % IMAGE)
    angle = reduced.astype(jnp.float32) * (2.0 * math.pi / IMAGE)
    return (jnp.cos(angle), jnp.sin(angle))

def matmul(left, right):
    return jnp.dot(left.astype(jnp.float32), right.astype(jnp.float32), precision=lax.Precision.HIGHEST)

def einsum_exact(form, left, right):
    return jnp.einsum(form, left.astype(jnp.float32), right.astype(jnp.float32), precision=lax.Precision.HIGHEST)

def reference(facets, window, facet_offsets, row_offsets, column_offset, kernel, tile_counts):
    cells = jnp.arange(FACET, dtype=jnp.int32)
    frequencies = jnp.arange(CONTRIB, dtype=jnp.int32)
    row_freqs = (row_offsets[:, None] + frequencies[None, :]).reshape(SUBGRIDS * CONTRIB)
    a_scale = 1.0 / math.sqrt(FACET * FACETS)
    b_scale = 1.0 / math.sqrt(FACET)
    back_scale = 1.0 / math.sqrt(SUBGRIDS * CONTRIB)
    out_scale = 1.0 / math.sqrt(CONTRIB)
    images = facets.reshape(FACETS, FACET, FACET)

    def column_tables(offset_y):
        return phase_table(column_offset[0] + frequencies[:, None], offset_y + cells[None, :])

    def forward(total, item):
        image, offset = item
        cosine, sine = column_tables(offset[1])
        col_real = (cosine * window[None, :] * b_scale).astype(jnp.bfloat16)
        col_imag = (-sine * window[None, :] * b_scale).astype(jnp.bfloat16)
        t_real = matmul(image, col_real.T).astype(jnp.bfloat16)
        t_imag = matmul(image, col_imag.T).astype(jnp.bfloat16)
        row_cos, row_sin = phase_table(row_freqs[:, None], offset[0] + cells[None, :])
        a_real = (row_cos * a_scale).astype(jnp.bfloat16)
        a_imag = (-row_sin * a_scale).astype(jnp.bfloat16)
        part_real = matmul(a_real, t_real) - matmul(a_imag, t_imag)
        part_imag = matmul(a_real, t_imag) + matmul(a_imag, t_real)
        return (total + jnp.stack([part_real, part_imag]), None)
    start_total = jnp.zeros((2, SUBGRIDS * CONTRIB, CONTRIB), jnp.float32)
    summed, _ = lax.scan(forward, start_total, (images, facet_offsets))
    grids = summed.reshape(2, SUBGRIDS, CONTRIB, CONTRIB).astype(jnp.bfloat16)
    tiles = CONTRIB // TILE
    counts = tile_counts.astype(jnp.float32)
    ratio = counts / (counts + 4.0)
    weights = jnp.broadcast_to(ratio[:, :, None, :, None], (SUBGRIDS, tiles, TILE, tiles, TILE))
    weights = weights.reshape(SUBGRIDS, CONTRIB, CONTRIB)
    y_grid = einsum_exact('csij,kj->csik', grids, kernel).astype(jnp.bfloat16)
    z_grid = einsum_exact('ki,csil->cskl', kernel, y_grid)
    w_grid = (weights[None] * z_grid).astype(jnp.bfloat16)
    u_grid = einsum_exact('jk,csjl->cskl', kernel, w_grid).astype(jnp.bfloat16)
    r_grid = einsum_exact('csij,jl->csil', u_grid, kernel).astype(jnp.bfloat16)
    stacked = r_grid.reshape(2, SUBGRIDS * CONTRIB, CONTRIB)

    def backward(offset):
        row_cos, row_sin = phase_table(row_freqs[:, None], offset[0] + cells[None, :])
        back_real = (row_cos * back_scale).astype(jnp.bfloat16)
        back_imag = (row_sin * back_scale).astype(jnp.bfloat16)
        e_real = matmul(back_real.T, stacked[0]) - matmul(back_imag.T, stacked[1])
        e_imag = matmul(back_real.T, stacked[1]) + matmul(back_imag.T, stacked[0])
        cosine, sine = column_tables(offset[1])
        out_cos = (cosine * out_scale).astype(jnp.bfloat16)
        out_sin = (sine * out_scale).astype(jnp.bfloat16)
        image = matmul(e_real.astype(jnp.bfloat16), out_cos) - matmul(e_imag.astype(jnp.bfloat16), out_sin)
        return (window[None, :] * image).astype(jnp.bfloat16)
    result = lax.map(backward, facet_offsets)
    return result.reshape(FACETS * FACET, FACET)
```

```python
import math

import jax
import jax.numpy as jnp
import numpy as np
from jax import lax
from jax.experimental import pallas as pl
from jax.experimental.pallas import tpu as pltpu
from jax.sharding import Mesh
from jax.sharding import PartitionSpec as P

IMAGE = 49152
STEP = 16
PLANE = ("y", "x")
DEPTH = ("zh", "zl")
ROWS = ("y", "zh", "x", "zl")


def wrapped(value):
    return jnp.where(value >= IMAGE, value - IMAGE, value)


def unit_circle(first, second):
    whole = first * second
    upper = lax.shift_right_logical(whole, jnp.int32(14))
    thirds = jnp.floor((upper.astype(jnp.float32) + 0.5) * (1.0 / 3.0)).astype(jnp.int32)
    reduced = (whole & 16383) + ((upper - 3 * thirds) << 14)
    turns = reduced.astype(jnp.float32)
    quarter = jnp.floor(turns * (4.0 / IMAGE) + 0.5)
    angle = (turns - quarter * (IMAGE / 4)) * (2.0 * math.pi / IMAGE)
    q = quarter.astype(jnp.int32)
    z = angle * angle
    sine = angle + angle * z * (
        -1.6666654611e-1 + z * (8.3321608736e-3 + z * -1.9515295891e-4)
    )
    cosine = 1.0 - 0.5 * z + z * z * (
        4.166664568298827e-2 + z * (-1.388731625493765e-3 + z * 2.443315711809948e-5)
    )
    odd = (q & 1) == 1
    c = jnp.where(odd, sine, cosine)
    s = jnp.where(odd, cosine, sine)
    c = jnp.where(((q + 1) & 2) == 2, -c, c)
    s = jnp.where((q & 2) == 2, -s, s)
    return c, s


def iota(shape, dim):
    return lax.broadcasted_iota(jnp.int32, shape, dim)


def nt(a, b):
    return lax.dot_general(a, b, (((1,), (1,)), ((), ())), preferred_element_type=jnp.float32)


def nn(a, b):
    return lax.dot_general(a, b, (((1,), (0,)), ((), ())), preferred_element_type=jnp.float32)


def forward_kernel(
    where_ref, offs_ref, rows_ref, col_ref, window_ref, facet_ref,
    part_ref, a_ref, d_ref, b_scr, t_scr,
    *, bands, subs, per, contrib, a_scale, b_scale, d_scale,
):
    me = where_ref[0]
    facet_at = me // (bands * subs)
    band_at = (me // subs) % bands
    sub_at = me % subs
    ox = offs_ref[facet_at, 0]
    oy = offs_ref[facet_at, 1]
    nx, ny = facet_ref.shape
    blocks = contrib // STEP

    v = wrapped(oy + iota((STEP, ny), 1))
    small_c, small_s = unit_circle(iota((STEP, ny), 0), v)
    big_c, big_s = unit_circle(wrapped(col_ref[0] + STEP * iota((blocks, ny), 0)), v)
    taper = window_ref[...]
    for a in range(blocks):
        gc, gs = big_c[a : a + 1], big_s[a : a + 1]
        c = gc * small_c - gs * small_s
        s = gc * small_s + gs * small_c
        lo = a * STEP
        b_scr[lo : lo + STEP, :] = (c * taper * b_scale).astype(jnp.bfloat16)
        b_scr[contrib + lo : contrib + lo + STEP, :] = (-s * taper * b_scale).astype(jnp.bfloat16)
        d_ref[lo : lo + STEP, :] = (c * d_scale).astype(jnp.bfloat16)
        d_ref[contrib + lo : contrib + lo + STEP, :] = (-s * d_scale).astype(jnp.bfloat16)
    t = nt(b_scr[...], facet_ref[...])
    tr = t[:contrib].astype(jnp.bfloat16)
    ti = t[contrib:].astype(jnp.bfloat16)
    t_scr[0, :contrib, :] = tr
    t_scr[0, contrib:, :] = ti
    t_scr[1, :contrib, :] = -ti
    t_scr[1, contrib:, :] = tr

    v = wrapped(ox + band_at * nx + iota((STEP, nx), 1))
    small_c, small_s = unit_circle(iota((STEP, nx), 0), v)
    small_c = small_c * a_scale
    small_s = small_s * a_scale
    for s_at in range(per):
        start = rows_ref[sub_at * per + s_at]
        big_c, big_s = unit_circle(wrapped(start + STEP * iota((blocks, nx), 0)), v)
        for a in range(blocks):
            gc, gs = big_c[a : a + 1], big_s[a : a + 1]
            c = gc * small_c - gs * small_s
            s = gc * small_s + gs * small_c
            a_ref[s_at, 0, a * STEP : (a + 1) * STEP, :] = c.astype(jnp.bfloat16)
            a_ref[s_at, 1, a * STEP : (a + 1) * STEP, :] = (-s).astype(jnp.bfloat16)
        part = nt(t_scr[0], a_ref[s_at, 0]) + nt(t_scr[1], a_ref[s_at, 1])
        part_ref[0, s_at] = part[:contrib].astype(jnp.bfloat16)
        part_ref[1, s_at] = part[contrib:].astype(jnp.bfloat16)


def middle_kernel(
    where_ref, grid_ref, a_ref, kern_ref, kern_t_ref, counts_ref, e_ref,
    y_scr, w_scr, r_scr, *, subs, per, contrib, tile,
):
    sub_at = where_ref[0] % subs
    tiles = contrib // tile
    k = kern_ref[...]
    kt = kern_t_ref[...]
    spread = (iota((tiles, contrib), 1) // tile == iota((tiles, contrib), 0)).astype(jnp.bfloat16)
    for c in range(2):
        for s in range(per):
            y_scr[c, s] = nn(k, grid_ref[c, s]).astype(jnp.bfloat16)
    for s in range(per):
        count = nn(counts_ref[sub_at * per + s], spread)
        weight = (count / (count + 4.0))[:, None, :]
        for c in range(2):
            z = nt(y_scr[c, s], k).reshape(tiles, tile, contrib)
            w_scr[c, s] = (weight * z).reshape(contrib, contrib).astype(jnp.bfloat16)
    for s in range(per):
        for c in range(2):
            u = nn(w_scr[c, s], k).astype(jnp.bfloat16)
            r_scr[s, c] = nn(kt, u).astype(jnp.bfloat16)
    total = None
    for s in range(per):
        rr = r_scr[s, 0]
        ri = r_scr[s, 1]
        here = nn(jnp.concatenate([rr, ri], 0), a_ref[s, 0])
        here = here + nn(jnp.concatenate([ri, -rr], 0), a_ref[s, 1])
        total = here if total is None else total + here
    e_ref[...] = total.T.astype(jnp.bfloat16)


def backward_kernel(mine_ref, other_ref, d_ref, window_ref, out_ref):
    e = (mine_ref[...].astype(jnp.float32) + other_ref[...].astype(jnp.float32)).astype(jnp.bfloat16)
    image = nn(e, d_ref[...])
    out_ref[...] = (window_ref[...] * image).astype(jnp.bfloat16)


def exchanged(x, axes):
    return lax.all_to_all(x, axes, 0, 0, tiled=True)


def summed(x):
    return jnp.sum(x.astype(jnp.float32), axis=0).astype(jnp.bfloat16)


def body(facets, window, facet_offsets, row_offsets, column_offset, kernel, tile_counts):
    bands, subs = lax.axis_size("zl"), lax.axis_size("core")
    plane, depth = lax.axis_size(PLANE), lax.axis_size(DEPTH)
    facet_count = plane * depth // bands
    nx, ny = facets.shape
    contrib = kernel.shape[0]
    per = row_offsets.shape[0] // subs
    tile = contrib // tile_counts.shape[1]
    a_scale = 1.0 / math.sqrt(ny * facet_count)
    b_scale = 1.0 / math.sqrt(ny)
    back_scale = 1.0 / math.sqrt(row_offsets.shape[0] * contrib)
    d_scale = back_scale / a_scale / math.sqrt(contrib)
    here = lax.axis_index(ROWS + ("core",)).astype(jnp.int32).reshape(1)
    taper = window.reshape(1, ny)
    smem = pl.BlockSpec(memory_space=pltpu.SMEM)
    vmem = pl.BlockSpec(memory_space=pltpu.VMEM)

    part, a_table, d_table = pl.pallas_call(
        lambda *refs: forward_kernel(
            *refs, bands=bands, subs=subs, per=per, contrib=contrib,
            a_scale=a_scale, b_scale=b_scale, d_scale=d_scale,
        ),
        out_shape=(
            jax.ShapeDtypeStruct((2, per, contrib, contrib), jnp.bfloat16),
            jax.ShapeDtypeStruct((per, 2, contrib, nx), jnp.bfloat16),
            jax.ShapeDtypeStruct((2 * contrib, ny), jnp.bfloat16),
        ),
        in_specs=[smem, smem, smem, smem, vmem, vmem],
        out_specs=(vmem, vmem, vmem),
        scratch_shapes=[
            pltpu.VMEM((2 * contrib, ny), jnp.bfloat16),
            pltpu.VMEM((2, 2 * contrib, nx), jnp.bfloat16),
        ],
        name="forward",
    )(here, facet_offsets, row_offsets, column_offset, taper, facets)

    lines = 2 * per * contrib
    mine = summed(exchanged(part.reshape(plane, lines // plane, contrib), PLANE))
    mine = summed(exchanged(mine.reshape(depth, lines // plane // depth, contrib), DEPTH))
    mine = exchanged(jnp.broadcast_to(mine, (depth, *mine.shape)), DEPTH)
    mine = mine.reshape(lines // plane, contrib)
    grid = exchanged(jnp.broadcast_to(mine, (plane, *mine.shape)), PLANE)
    grid = grid.reshape(2, per, contrib, contrib)

    counts = jnp.swapaxes(tile_counts, 1, 2).astype(jnp.bfloat16)
    e_part = pl.pallas_call(
        lambda *refs: middle_kernel(*refs, subs=subs, per=per, contrib=contrib, tile=tile),
        out_shape=jax.ShapeDtypeStruct((nx, 2 * contrib), jnp.bfloat16),
        in_specs=[smem, vmem, vmem, vmem, vmem, vmem],
        out_specs=vmem,
        scratch_shapes=[
            pltpu.VMEM((2, per, contrib, contrib), jnp.bfloat16),
            pltpu.VMEM((2, per, contrib, contrib), jnp.bfloat16),
            pltpu.VMEM((per, 2, contrib, contrib), jnp.bfloat16),
        ],
        name="middle",
    )(here, grid, a_table, kernel, kernel.T, counts)

    other = lax.ppermute(e_part, "core", [(i, (i + 1) % subs) for i in range(subs)])
    step = nx // 4
    return pl.pallas_call(
        backward_kernel,
        out_shape=jax.ShapeDtypeStruct((nx, ny), jnp.bfloat16),
        grid=(nx // step,),
        in_specs=[
            pl.BlockSpec((step, 2 * contrib), lambda i: (i, 0)),
            pl.BlockSpec((step, 2 * contrib), lambda i: (i, 0)),
            pl.BlockSpec((2 * contrib, ny), lambda i: (0, 0)),
            pl.BlockSpec((1, ny), lambda i: (0, 0)),
        ],
        out_specs=pl.BlockSpec((step, ny), lambda i: (i, 0)),
        name="backward",
    )(e_part, other, d_table, taper)


def solution(mesh):
    fine = Mesh(np.asarray(mesh.devices).reshape(4, 4, 4, 4, 2), ROWS + ("core",))
    rows = P(ROWS, None)
    return jax.shard_map(
        body,
        mesh=fine,
        in_specs=(rows, P(), P(), P(), P(), P(), P()),
        out_specs=rows,
        check_vma=False,
    )
```

```python
import math

import jax
import jax.numpy as jnp
import numpy as np
from jax import lax
from jax.experimental import pallas as pl
from jax.experimental.pallas import tpu as pltpu
from jax.sharding import Mesh
from jax.sharding import PartitionSpec as P

IMAGE = 49152
STEP = 16
PLANE = ("y", "x")
DEPTH = ("zh", "zl")
ROWS = ("y", "zh", "x", "zl")


def wrapped(value):
    return jnp.where(value >= IMAGE, value - IMAGE, value)


def unit_circle(first, second):
    whole = first * second
    upper = lax.shift_right_logical(whole, jnp.int32(14))
    thirds = jnp.floor((upper.astype(jnp.float32) + 0.5) * (1.0 / 3.0)).astype(jnp.int32)
    reduced = (whole & 16383) + ((upper - 3 * thirds) << 14)
    turns = reduced.astype(jnp.float32)
    quarter = jnp.floor(turns * (4.0 / IMAGE) + 0.5)
    angle = (turns - quarter * (IMAGE / 4)) * (2.0 * math.pi / IMAGE)
    q = quarter.astype(jnp.int32)
    z = angle * angle
    sine = angle + angle * z * (
        -1.6666654611e-1 + z * (8.3321608736e-3 + z * -1.9515295891e-4)
    )
    cosine = 1.0 - 0.5 * z + z * z * (
        4.166664568298827e-2 + z * (-1.388731625493765e-3 + z * 2.443315711809948e-5)
    )
    odd = (q & 1) == 1
    c = jnp.where(odd, sine, cosine)
    s = jnp.where(odd, cosine, sine)
    c = jnp.where(((q + 1) & 2) == 2, -c, c)
    s = jnp.where((q & 2) == 2, -s, s)
    return c, s


def iota(shape, dim):
    return lax.broadcasted_iota(jnp.int32, shape, dim)


def nt(a, b):
    return lax.dot_general(a, b, (((1,), (1,)), ((), ())), preferred_element_type=jnp.float32)


def nn(a, b):
    return lax.dot_general(a, b, (((1,), (0,)), ((), ())), preferred_element_type=jnp.float32)


def turned(big_c, big_s, a, small_c, small_s):
    gc, gs = big_c[a : a + 1], big_s[a : a + 1]
    return gc * small_c - gs * small_s, gc * small_s + gs * small_c


def place(where_ref, bands, subs):
    me = where_ref[0]
    return me // (bands * subs), (me // subs) % bands, me % subs


def column_factors(oy, start, blocks, ny):
    v = wrapped(oy + iota((STEP, ny), 1))
    return unit_circle(iota((STEP, ny), 0), v), unit_circle(
        wrapped(start + STEP * iota((blocks, ny), 0)), v
    )


def row_table(start, v, small, blocks, store):
    big_c, big_s = unit_circle(wrapped(start + STEP * iota((blocks, v.shape[1]), 0)), v)
    for a in range(blocks):
        c, s = turned(big_c, big_s, a, *small)
        store(a * STEP, c.astype(jnp.bfloat16), (-s).astype(jnp.bfloat16))


def forward_kernel(
    where_ref, offs_ref, rows_ref, col_ref, window_ref, facet_hbm,
    part_ref, facet_scr, b_scr, t_scr, a_scr, sem,
    *, bands, subs, per, contrib, a_scale, b_scale,
):
    load = pltpu.make_async_copy(facet_hbm, facet_scr, sem)
    load.start()
    facet_at, band_at, sub_at = place(where_ref, bands, subs)
    ox = offs_ref[0, facet_at]
    oy = offs_ref[1, facet_at]
    nx, ny = facet_scr.shape
    blocks = contrib // STEP

    small, (big_c, big_s) = column_factors(oy, col_ref[0], blocks, ny)
    taper = window_ref[...] * b_scale
    small = (small[0] * taper, small[1] * taper)
    for a in range(blocks):
        c, s = turned(big_c, big_s, a, *small)
        lo = a * STEP
        b_scr[lo : lo + STEP, :] = c.astype(jnp.bfloat16)
        b_scr[contrib + lo : contrib + lo + STEP, :] = (-s).astype(jnp.bfloat16)
    load.wait()
    t = nt(b_scr[...], facet_scr[...])
    tr = t[:contrib].astype(jnp.bfloat16)
    ti = t[contrib:].astype(jnp.bfloat16)
    t_scr[0, :contrib, :] = tr
    t_scr[0, contrib:, :] = ti
    t_scr[1, :contrib, :] = -ti
    t_scr[1, contrib:, :] = tr

    v = wrapped(ox + band_at * nx + iota((STEP, nx), 1))
    small_c, small_s = unit_circle(iota((STEP, nx), 0), v)
    small = (small_c * a_scale, small_s * a_scale)
    for s_at in range(per):

        def store(lo, c, s):
            a_scr[s_at, 0, lo : lo + STEP, :] = c
            a_scr[s_at, 1, lo : lo + STEP, :] = s

        row_table(rows_ref[sub_at * per + s_at], v, small, blocks, store)
    for s_at in range(per):
        part = nt(t_scr[0], a_scr[s_at, 0]) + nt(t_scr[1], a_scr[s_at, 1])
        part_ref[0, s_at] = part[:contrib].astype(jnp.bfloat16)
        part_ref[1, s_at] = part[contrib:].astype(jnp.bfloat16)


def tables_kernel(
    where_ref, offs_ref, rows_ref, col_ref, kern_ref, after_ref, a_ref, d_ref, kern_t_ref,
    *, bands, subs, per, contrib, a_scale, d_scale,
):
    del after_ref
    facet_at, band_at, sub_at = place(where_ref, bands, subs)
    ox = offs_ref[0, facet_at]
    oy = offs_ref[1, facet_at]
    nx, ny = a_ref.shape[3], d_ref.shape[1]
    blocks = contrib // STEP
    kern_t_ref[...] = kern_ref[...].astype(jnp.float32).T.astype(jnp.bfloat16)
    small, (big_c, big_s) = column_factors(oy, col_ref[0], blocks, ny)
    small = (small[0] * d_scale, small[1] * d_scale)
    for a in range(blocks):
        c, s = turned(big_c, big_s, a, *small)
        lo = a * STEP
        d_ref[lo : lo + STEP, :] = c.astype(jnp.bfloat16)
        d_ref[contrib + lo : contrib + lo + STEP, :] = (-s).astype(jnp.bfloat16)
    v = wrapped(ox + band_at * nx + iota((STEP, nx), 1))
    small_c, small_s = unit_circle(iota((STEP, nx), 0), v)
    small = (small_c * a_scale, small_s * a_scale)
    for s_at in range(per):

        def store(lo, c, s):
            a_ref[s_at, 0, lo : lo + STEP, :] = c
            a_ref[s_at, 1, lo : lo + STEP, :] = s

        row_table(rows_ref[sub_at * per + s_at], v, small, blocks, store)


def middle_kernel(
    where_ref, grid_ref, a_hbm, kern_ref, kern_t_ref, counts_ref, e_ref,
    a_ref, y_scr, w_scr, r_scr, sem, *, subs, per, contrib, tile,
):
    load = pltpu.make_async_copy(a_hbm, a_ref, sem)
    load.start()
    sub_at = where_ref[0] % subs
    tiles = contrib // tile
    k = kern_ref[...]
    kt = kern_t_ref[...]
    spread = (iota((tiles, contrib), 1) // tile == iota((tiles, contrib), 0)).astype(jnp.bfloat16)
    for c in range(2):
        for s in range(per):
            y_scr[c, s] = nn(k, grid_ref[c, s]).astype(jnp.bfloat16)
    for s in range(per):
        count = nn(counts_ref[sub_at * per + s], spread)
        weight = (count / (count + 4.0))[:, None, :]
        for c in range(2):
            z = nt(y_scr[c, s], k).reshape(tiles, tile, contrib)
            w_scr[c, s] = (weight * z).reshape(contrib, contrib).astype(jnp.bfloat16)
    for s in range(per):
        for c in range(2):
            u = nn(w_scr[c, s], k).astype(jnp.bfloat16)
            r_scr[s, c] = nn(kt, u).astype(jnp.bfloat16)
    load.wait()
    total = None
    for s in range(per):
        rr = r_scr[s, 0]
        ri = r_scr[s, 1]
        here = nn(jnp.concatenate([rr, ri], 0), a_ref[s, 0])
        here = here + nn(jnp.concatenate([ri, -rr], 0), a_ref[s, 1])
        total = here if total is None else total + here
    e_ref[...] = total.T.astype(jnp.bfloat16)


def backward_kernel(mine_ref, other_ref, d_ref, window_ref, out_ref, e_scr, *, cols):
    at = pl.program_id(0)

    @pl.when(at == 0)
    def _():
        e_scr[...] = (
            mine_ref[...].astype(jnp.float32) + other_ref[...].astype(jnp.float32)
        ).astype(jnp.bfloat16)

    here = pl.ds(pl.multiple_of(at * cols, cols), cols)
    image = nn(e_scr[...], d_ref[:, here])
    out_ref[...] = (window_ref[:, here] * image).astype(jnp.bfloat16)


def exchanged(x, axes):
    return lax.all_to_all(x, axes, 0, 0, tiled=True)


def summed(x):
    return jnp.sum(x.astype(jnp.float32), axis=0).astype(jnp.bfloat16)


def near(x):
    return pltpu.with_memory_space_constraint(x, pltpu.VMEM)


def body(facets, window, facet_offsets, row_offsets, column_offset, kernel, tile_counts):
    bands, subs = lax.axis_size("zl"), lax.axis_size("core")
    plane, depth = lax.axis_size(PLANE), lax.axis_size(DEPTH)
    facet_count = plane * depth // bands
    nx, ny = facets.shape
    contrib = kernel.shape[0]
    per = row_offsets.shape[0] // subs
    tile = contrib // tile_counts.shape[1]
    a_scale = 1.0 / math.sqrt(ny * facet_count)
    b_scale = 1.0 / math.sqrt(ny)
    back_scale = 1.0 / math.sqrt(row_offsets.shape[0] * contrib)
    d_scale = back_scale / a_scale / math.sqrt(contrib)
    here = lax.axis_index(ROWS + ("core",)).astype(jnp.int32).reshape(1)
    taper = window.reshape(1, ny)
    offsets = facet_offsets.T
    smem = pl.BlockSpec(memory_space=pltpu.SMEM)
    vmem = pl.BlockSpec(memory_space=pltpu.VMEM)
    anywhere = pl.BlockSpec(memory_space=pl.ANY)
    far = pl.BlockSpec(memory_space=pltpu.HBM)

    part = pl.pallas_call(
        lambda *refs: forward_kernel(
            *refs, bands=bands, subs=subs, per=per, contrib=contrib, a_scale=a_scale, b_scale=b_scale,
        ),
        out_shape=pltpu.VMEM((2, per, contrib, contrib), jnp.bfloat16),
        in_specs=[smem, smem, smem, smem, vmem, far],
        out_specs=vmem,
        scratch_shapes=[
            pltpu.VMEM((nx, ny), jnp.bfloat16),
            pltpu.VMEM((2 * contrib, ny), jnp.bfloat16),
            pltpu.VMEM((2, 2 * contrib, nx), jnp.bfloat16),
            pltpu.VMEM((per, 2, contrib, nx), jnp.bfloat16),
            pltpu.SemaphoreType.DMA(()),
        ],
        compiler_params=pltpu.CompilerParams(vmem_limit_bytes=28 * 2**20),
        name="forward",
    )(here, offsets, row_offsets, column_offset, taper, pltpu.with_memory_space_constraint(facets, pltpu.HBM))

    lines = 2 * per * contrib
    mine = summed(exchanged(part.reshape(plane, lines // plane, contrib), PLANE))
    a_table, d_table, kernel_t = pl.pallas_call(
        lambda *refs: tables_kernel(
            *refs, bands=bands, subs=subs, per=per, contrib=contrib, a_scale=a_scale, d_scale=d_scale,
        ),
        out_shape=(
            pltpu.HBM((per, 2, contrib, nx), jnp.bfloat16),
            pltpu.VMEM((2 * contrib, ny), jnp.bfloat16),
            pltpu.VMEM((contrib, contrib), jnp.bfloat16),
        ),
        in_specs=[smem, smem, smem, smem, vmem, anywhere],
        out_specs=(vmem, vmem, vmem),
        cost_estimate=pl.CostEstimate(flops=6_000_000_000, transcendentals=0, bytes_accessed=4_000_000),
        compiler_params=pltpu.CompilerParams(vmem_limit_bytes=20 * 2**20),
        name="tables",
    )(here, offsets, row_offsets, column_offset, kernel, mine)
    mine = summed(exchanged(mine.reshape(depth, lines // plane // depth, contrib), DEPTH))
    mine = exchanged(jnp.broadcast_to(mine, (depth, *mine.shape)), DEPTH)
    mine = mine.reshape(lines // plane, contrib)
    grid = exchanged(jnp.broadcast_to(mine, (plane, *mine.shape)), PLANE)
    grid = grid.reshape(2, per, contrib, contrib)

    counts = jnp.swapaxes(tile_counts, 1, 2).astype(jnp.bfloat16)
    e_part = pl.pallas_call(
        lambda *refs: middle_kernel(*refs, subs=subs, per=per, contrib=contrib, tile=tile),
        out_shape=pltpu.VMEM((nx, 2 * contrib), jnp.bfloat16),
        in_specs=[smem, vmem, far, vmem, vmem, vmem],
        out_specs=vmem,
        scratch_shapes=[
            pltpu.VMEM((per, 2, contrib, nx), jnp.bfloat16),
            pltpu.VMEM((2, per, contrib, contrib), jnp.bfloat16),
            pltpu.VMEM((2, per, contrib, contrib), jnp.bfloat16),
            pltpu.VMEM((per, 2, contrib, contrib), jnp.bfloat16),
            pltpu.SemaphoreType.DMA(()),
        ],
        compiler_params=pltpu.CompilerParams(vmem_limit_bytes=28 * 2**20),
        name="middle",
    )(here, near(grid), pltpu.with_memory_space_constraint(a_table, pltpu.HBM), kernel, near(kernel_t), counts)

    other = lax.ppermute(e_part, "core", [(i, (i + 1) % subs) for i in range(subs)])
    cols = ny // 4
    return pl.pallas_call(
        lambda *refs: backward_kernel(*refs, cols=cols),
        out_shape=jax.ShapeDtypeStruct((nx, ny), jnp.bfloat16),
        grid=(ny // cols,),
        in_specs=[vmem, vmem, vmem, vmem],
        out_specs=pl.BlockSpec((nx, cols), lambda i: (0, i)),
        scratch_shapes=[pltpu.VMEM((nx, 2 * contrib), jnp.bfloat16)],
        compiler_params=pltpu.CompilerParams(vmem_limit_bytes=28 * 2**20),
        name="backward",
    )(near(e_part), near(other), near(d_table), taper)


def solution(mesh):
    fine = Mesh(np.asarray(mesh.devices).reshape(4, 4, 4, 4, 2), ROWS + ("core",))
    rows = P(ROWS, None)
    return jax.shard_map(
        body,
        mesh=fine,
        in_specs=(rows, P(), P(), P(), P(), P(), P()),
        out_specs=rows,
        check_vma=False,
    )
```

```python
import math

import jax
import jax.numpy as jnp
import numpy as np
from jax import lax
from jax.experimental import pallas as pl
from jax.experimental.pallas import tpu as pltpu
from jax.sharding import Mesh
from jax.sharding import PartitionSpec as P

IMAGE = 49152
STEP = 16
PLANE = ("y", "x")
DEPTH = ("zh", "zl")
ROWS = ("y", "zh", "x", "zl")


def wrapped(value):
    return jnp.where(value >= IMAGE, value - IMAGE, value)


def unit_circle(first, second):
    whole = first * second
    upper = lax.shift_right_logical(whole, jnp.int32(14))
    thirds = jnp.floor((upper.astype(jnp.float32) + 0.5) * (1.0 / 3.0)).astype(jnp.int32)
    reduced = (whole & 16383) + ((upper - 3 * thirds) << 14)
    turns = reduced.astype(jnp.float32)
    quarter = jnp.floor(turns * (4.0 / IMAGE) + 0.5)
    angle = (turns - quarter * (IMAGE / 4)) * (2.0 * math.pi / IMAGE)
    q = quarter.astype(jnp.int32)
    z = angle * angle
    sine = angle + angle * z * (
        -1.6666654611e-1 + z * (8.3321608736e-3 + z * -1.9515295891e-4)
    )
    cosine = 1.0 - 0.5 * z + z * z * (
        4.166664568298827e-2 + z * (-1.388731625493765e-3 + z * 2.443315711809948e-5)
    )
    odd = (q & 1) == 1
    c = jnp.where(odd, sine, cosine)
    s = jnp.where(odd, cosine, sine)
    c = jnp.where(((q + 1) & 2) == 2, -c, c)
    s = jnp.where((q & 2) == 2, -s, s)
    return c, s


def iota(shape, dim):
    return lax.broadcasted_iota(jnp.int32, shape, dim)


def nt(a, b):
    return lax.dot_general(a, b, (((1,), (1,)), ((), ())), preferred_element_type=jnp.float32)


def nn(a, b):
    return lax.dot_general(a, b, (((1,), (0,)), ((), ())), preferred_element_type=jnp.float32)


def turned(big_c, big_s, a, small_c, small_s):
    gc, gs = big_c[a : a + 1], big_s[a : a + 1]
    return gc * small_c - gs * small_s, gc * small_s + gs * small_c


def place(where_ref, bands, subs):
    me = where_ref[0]
    return me // (bands * subs), (me // subs) % bands, me % subs


def column_factors(oy, start, blocks, ny):
    v = wrapped(oy + iota((STEP, ny), 1))
    return unit_circle(iota((STEP, ny), 0), v), unit_circle(
        wrapped(start + STEP * iota((blocks, ny), 0)), v
    )


def row_table(start, v, small, blocks, store):
    big_c, big_s = unit_circle(wrapped(start + STEP * iota((blocks, v.shape[1]), 0)), v)
    for a in range(blocks):
        c, s = turned(big_c, big_s, a, *small)
        store(a * STEP, c.astype(jnp.bfloat16), (-s).astype(jnp.bfloat16))


def forward_kernel(
    where_ref, offs_ref, rows_ref, col_ref, window_ref, facet_hbm,
    part_ref, facet_scr, b_scr, t_scr, a_scr, sem,
    *, bands, subs, per, contrib, a_scale, b_scale,
):
    load = pltpu.make_async_copy(facet_hbm, facet_scr, sem)
    load.start()
    facet_at, band_at, sub_at = place(where_ref, bands, subs)
    ox = offs_ref[0, facet_at]
    oy = offs_ref[1, facet_at]
    nx, ny = facet_scr.shape
    blocks = contrib // STEP

    width = min(256, ny)

    def columns(at, carry):
        lanes = pl.ds(pl.multiple_of(at * width, width), width)
        small, big = column_factors(oy + at * width, col_ref[0], blocks, width)
        taper = window_ref[:, lanes] * b_scale
        small = (small[0] * taper, small[1] * taper)
        for a in range(blocks):
            c, s = turned(*big, a, *small)
            lo = a * STEP
            b_scr[lo : lo + STEP, lanes] = c.astype(jnp.bfloat16)
            b_scr[contrib + lo : contrib + lo + STEP, lanes] = (-s).astype(jnp.bfloat16)
        return carry

    lax.fori_loop(0, ny // width, columns, 0)
    load.wait()

    v = wrapped(ox + band_at * nx + iota((STEP, nx), 1))
    small_c, small_s = unit_circle(iota((STEP, nx), 0), v)
    small = (small_c * a_scale, small_s * a_scale)
    for s_at in range(per):

        def store(lo, c, s):
            a_scr[s_at, 0, lo : lo + STEP, :] = c
            a_scr[s_at, 1, lo : lo + STEP, :] = s

        row_table(rows_ref[sub_at * per + s_at], v, small, blocks, store)
    t = nt(b_scr[...], facet_scr[...])
    tr = t[:contrib].astype(jnp.bfloat16)
    ti = t[contrib:].astype(jnp.bfloat16)
    t_scr[0, :contrib, :] = tr
    t_scr[0, contrib:, :] = ti
    t_scr[1, :contrib, :] = -ti
    t_scr[1, contrib:, :] = tr
    for s_at in range(per):
        part = nt(t_scr[0], a_scr[s_at, 0]) + nt(t_scr[1], a_scr[s_at, 1])
        part_ref[0, s_at] = part[:contrib].astype(jnp.bfloat16)
        part_ref[1, s_at] = part[contrib:].astype(jnp.bfloat16)


def tables_kernel(
    where_ref, offs_ref, rows_ref, col_ref, kern_ref, after_ref, a_ref, d_ref, kern_t_ref,
    *, bands, subs, per, contrib, a_scale, d_scale,
):
    del after_ref
    facet_at, band_at, sub_at = place(where_ref, bands, subs)
    ox = offs_ref[0, facet_at]
    oy = offs_ref[1, facet_at]
    nx, ny = a_ref.shape[3], d_ref.shape[1]
    blocks = contrib // STEP
    kern_t_ref[...] = kern_ref[...].astype(jnp.float32).T.astype(jnp.bfloat16)
    small, (big_c, big_s) = column_factors(oy, col_ref[0], blocks, ny)
    small = (small[0] * d_scale, small[1] * d_scale)
    for a in range(blocks):
        c, s = turned(big_c, big_s, a, *small)
        lo = a * STEP
        d_ref[lo : lo + STEP, :] = c.astype(jnp.bfloat16)
        d_ref[contrib + lo : contrib + lo + STEP, :] = (-s).astype(jnp.bfloat16)
    v = wrapped(ox + band_at * nx + iota((STEP, nx), 1))
    small_c, small_s = unit_circle(iota((STEP, nx), 0), v)
    small = (small_c * a_scale, small_s * a_scale)
    for s_at in range(per):

        def store(lo, c, s):
            a_ref[s_at, 0, lo : lo + STEP, :] = c
            a_ref[s_at, 1, lo : lo + STEP, :] = s

        row_table(rows_ref[sub_at * per + s_at], v, small, blocks, store)


def middle_kernel(
    where_ref, grid_ref, a_hbm, kern_ref, kern_t_ref, counts_ref, e_ref,
    a_ref, y_scr, w_scr, r_scr, sem, *, subs, per, contrib, tile,
):
    load = pltpu.make_async_copy(a_hbm, a_ref, sem)
    load.start()
    sub_at = where_ref[0] % subs
    tiles = contrib // tile
    k = kern_ref[...]
    kt = kern_t_ref[...]
    spread = (iota((tiles, contrib), 1) // tile == iota((tiles, contrib), 0)).astype(jnp.bfloat16)
    for c in range(2):
        for s in range(per):
            y_scr[c, s] = nn(k, grid_ref[c, s]).astype(jnp.bfloat16)
    for s in range(per):
        count = nn(counts_ref[sub_at * per + s], spread)
        weight = (count / (count + 4.0))[:, None, :]
        for c in range(2):
            z = nt(y_scr[c, s], k).reshape(tiles, tile, contrib)
            w_scr[c, s] = (weight * z).reshape(contrib, contrib).astype(jnp.bfloat16)
    for s in range(per):
        for c in range(2):
            u = nn(w_scr[c, s], k).astype(jnp.bfloat16)
            r_scr[s, c] = nn(kt, u).astype(jnp.bfloat16)
    load.wait()
    total = None
    for s in range(per):
        rr = r_scr[s, 0]
        ri = r_scr[s, 1]
        here = nn(jnp.concatenate([rr, ri], 0), a_ref[s, 0])
        here = here + nn(jnp.concatenate([ri, -rr], 0), a_ref[s, 1])
        total = here if total is None else total + here
    e_ref[...] = total.T.astype(jnp.bfloat16)


def backward_kernel(mine_ref, other_ref, d_ref, window_ref, out_hbm, out_scr, sems, *, chunks):
    cols = out_scr.shape[1] // chunks
    e = (mine_ref[...].astype(jnp.float32) + other_ref[...].astype(jnp.float32)).astype(jnp.bfloat16)
    sends = []
    for j in range(chunks):
        here = slice(j * cols, (j + 1) * cols)
        image = nn(e, d_ref[:, here])
        out_scr[:, here] = (window_ref[:, here] * image).astype(jnp.bfloat16)
        send = pltpu.make_async_copy(
            out_scr.at[:, pl.ds(j * cols, cols)], out_hbm.at[:, pl.ds(j * cols, cols)], sems.at[j]
        )
        send.start()
        sends.append(send)
    for send in sends:
        send.wait()


def exchanged(x, axes):
    return lax.all_to_all(x, axes, 0, 0, tiled=True)


def summed(x):
    return jnp.sum(x.astype(jnp.float32), axis=0).astype(jnp.bfloat16)


def distant(x):
    return pltpu.with_memory_space_constraint(x, pltpu.HBM)


def near(x):
    return pltpu.with_memory_space_constraint(x, pltpu.VMEM)


def body(facets, window, facet_offsets, row_offsets, column_offset, kernel, tile_counts):
    bands, subs = lax.axis_size("zl"), lax.axis_size("core")
    plane, depth = lax.axis_size(PLANE), lax.axis_size(DEPTH)
    facet_count = plane * depth // bands
    nx, ny = facets.shape
    contrib = kernel.shape[0]
    per = row_offsets.shape[0] // subs
    tile = contrib // tile_counts.shape[1]
    a_scale = 1.0 / math.sqrt(ny * facet_count)
    b_scale = 1.0 / math.sqrt(ny)
    back_scale = 1.0 / math.sqrt(row_offsets.shape[0] * contrib)
    d_scale = back_scale / a_scale / math.sqrt(contrib)
    here = lax.axis_index(ROWS + ("core",)).astype(jnp.int32).reshape(1)
    taper = window.reshape(1, ny)
    offsets = facet_offsets.T
    smem = pl.BlockSpec(memory_space=pltpu.SMEM)
    vmem = pl.BlockSpec(memory_space=pltpu.VMEM)
    anywhere = pl.BlockSpec(memory_space=pl.ANY)
    far = pl.BlockSpec(memory_space=pltpu.HBM)

    part = pl.pallas_call(
        lambda *refs: forward_kernel(
            *refs, bands=bands, subs=subs, per=per, contrib=contrib, a_scale=a_scale, b_scale=b_scale,
        ),
        out_shape=pltpu.VMEM((2, per, contrib, contrib), jnp.bfloat16),
        in_specs=[smem, smem, smem, smem, vmem, far],
        out_specs=vmem,
        scratch_shapes=[
            pltpu.VMEM((nx, ny), jnp.bfloat16),
            pltpu.VMEM((2 * contrib, ny), jnp.bfloat16),
            pltpu.VMEM((2, 2 * contrib, nx), jnp.bfloat16),
            pltpu.VMEM((per, 2, contrib, nx), jnp.bfloat16),
            pltpu.SemaphoreType.DMA(()),
        ],
        compiler_params=pltpu.CompilerParams(vmem_limit_bytes=28 * 2**20),
        name="forward",
    )(here, distant(offsets), distant(row_offsets), column_offset, distant(taper), distant(facets))

    lines = 2 * per * contrib
    mine = summed(exchanged(part.reshape(plane, lines // plane, contrib), PLANE))
    a_table, d_table, kernel_t = pl.pallas_call(
        lambda *refs: tables_kernel(
            *refs, bands=bands, subs=subs, per=per, contrib=contrib, a_scale=a_scale, d_scale=d_scale,
        ),
        out_shape=(
            pltpu.HBM((per, 2, contrib, nx), jnp.bfloat16),
            pltpu.VMEM((2 * contrib, ny), jnp.bfloat16),
            pltpu.VMEM((contrib, contrib), jnp.bfloat16),
        ),
        in_specs=[smem, smem, smem, smem, vmem, anywhere],
        out_specs=(vmem, vmem, vmem),
        cost_estimate=pl.CostEstimate(flops=6_000_000_000, transcendentals=0, bytes_accessed=4_000_000),
        compiler_params=pltpu.CompilerParams(vmem_limit_bytes=20 * 2**20),
        name="tables",
    )(here, offsets, row_offsets, column_offset, kernel, mine)
    mine = summed(exchanged(mine.reshape(depth, lines // plane // depth, contrib), DEPTH))
    mine = exchanged(jnp.broadcast_to(mine, (depth, *mine.shape)), DEPTH)
    mine = mine.reshape(lines // plane, contrib)
    grid = exchanged(jnp.broadcast_to(mine, (plane, *mine.shape)), PLANE)
    grid = grid.reshape(2, per, contrib, contrib)

    counts = jnp.swapaxes(tile_counts, 1, 2).astype(jnp.bfloat16)
    e_part = pl.pallas_call(
        lambda *refs: middle_kernel(*refs, subs=subs, per=per, contrib=contrib, tile=tile),
        out_shape=pltpu.VMEM((nx, 2 * contrib), jnp.bfloat16),
        in_specs=[smem, vmem, far, vmem, vmem, vmem],
        out_specs=vmem,
        scratch_shapes=[
            pltpu.VMEM((per, 2, contrib, nx), jnp.bfloat16),
            pltpu.VMEM((2, per, contrib, contrib), jnp.bfloat16),
            pltpu.VMEM((2, per, contrib, contrib), jnp.bfloat16),
            pltpu.VMEM((per, 2, contrib, contrib), jnp.bfloat16),
            pltpu.SemaphoreType.DMA(()),
        ],
        compiler_params=pltpu.CompilerParams(vmem_limit_bytes=28 * 2**20),
        name="middle",
    )(here, near(grid), distant(a_table), kernel, near(kernel_t), counts)

    other = lax.ppermute(e_part, "core", [(i, (i + 1) % subs) for i in range(subs)])
    chunks = 4
    return pl.pallas_call(
        lambda *refs: backward_kernel(*refs, chunks=chunks),
        out_shape=jax.ShapeDtypeStruct((nx, ny), jnp.bfloat16),
        in_specs=[vmem, vmem, vmem, vmem],
        out_specs=far,
        scratch_shapes=[pltpu.VMEM((nx, ny), jnp.bfloat16), pltpu.SemaphoreType.DMA((chunks,))],
        compiler_params=pltpu.CompilerParams(vmem_limit_bytes=28 * 2**20),
        name="backward",
    )(near(e_part), near(other), near(d_table), taper)


def solution(mesh):
    fine = Mesh(np.asarray(mesh.devices).reshape(4, 4, 4, 4, 2), ROWS + ("core",))
    rows = P(ROWS, None)
    return jax.shard_map(
        body,
        mesh=fine,
        in_specs=(rows, P(), P(), P(), P(), P(), P()),
        out_specs=rows,
        check_vma=False,
    )
```

```python
import math

import jax
import jax.numpy as jnp
import numpy as np
from jax import lax
from jax.experimental import pallas as pl
from jax.experimental.pallas import tpu as pltpu
from jax.sharding import Mesh
from jax.sharding import PartitionSpec as P

IMAGE = 49152
STEP = 16
PLANE = ("y", "x")
DEPTH = ("zh", "zl")
ROWS = ("y", "zh", "x", "zl")


def wrapped(value):
    return jnp.where(value >= IMAGE, value - IMAGE, value)


def unit_circle(first, second):
    whole = first * second
    upper = lax.shift_right_logical(whole, jnp.int32(14))
    thirds = jnp.floor((upper.astype(jnp.float32) + 0.5) * (1.0 / 3.0)).astype(jnp.int32)
    reduced = (whole & 16383) + ((upper - 3 * thirds) << 14)
    turns = reduced.astype(jnp.float32)
    quarter = jnp.floor(turns * (4.0 / IMAGE) + 0.5)
    angle = (turns - quarter * (IMAGE / 4)) * (2.0 * math.pi / IMAGE)
    q = quarter.astype(jnp.int32)
    z = angle * angle
    sine = angle + angle * z * (
        -1.6666654611e-1 + z * (8.3321608736e-3 + z * -1.9515295891e-4)
    )
    cosine = 1.0 - 0.5 * z + z * z * (
        4.166664568298827e-2 + z * (-1.388731625493765e-3 + z * 2.443315711809948e-5)
    )
    odd = (q & 1) == 1
    c = jnp.where(odd, sine, cosine)
    s = jnp.where(odd, cosine, sine)
    c = jnp.where(((q + 1) & 2) == 2, -c, c)
    s = jnp.where((q & 2) == 2, -s, s)
    return c, s


def iota(shape, dim):
    return lax.broadcasted_iota(jnp.int32, shape, dim)


def nt(a, b):
    return lax.dot_general(a, b, (((1,), (1,)), ((), ())), preferred_element_type=jnp.float32)


def nn(a, b):
    return lax.dot_general(a, b, (((1,), (0,)), ((), ())), preferred_element_type=jnp.float32)


def turned(big_c, big_s, a, small_c, small_s):
    gc, gs = big_c[a : a + 1], big_s[a : a + 1]
    return gc * small_c - gs * small_s, gc * small_s + gs * small_c


def place(where_ref, bands, subs):
    me = where_ref[0]
    return me // (bands * subs), (me // subs) % bands, me % subs


def column_factors(oy, start, blocks, ny):
    v = wrapped(oy + iota((STEP, ny), 1))
    return unit_circle(iota((STEP, ny), 0), v), unit_circle(
        wrapped(start + STEP * iota((blocks, ny), 0)), v
    )


def row_table(start, v, small, blocks, store):
    big_c, big_s = unit_circle(wrapped(start + STEP * iota((blocks, v.shape[1]), 0)), v)
    for a in range(blocks):
        c, s = turned(big_c, big_s, a, *small)
        store(a * STEP, c.astype(jnp.bfloat16), (-s).astype(jnp.bfloat16))


def forward_kernel(
    where_ref, offs_ref, rows_ref, col_ref, window_ref, kern_ref, facet_hbm,
    part_ref, facet_scr, b_scr, t_scr, a_scr, sem,
    *, bands, subs, per, contrib, a_scale, b_scale,
):
    load = pltpu.make_async_copy(facet_hbm, facet_scr, sem)
    load.start()
    facet_at, band_at, sub_at = place(where_ref, bands, subs)
    ox = offs_ref[0, facet_at]
    oy = offs_ref[1, facet_at]
    nx, ny = facet_scr.shape
    blocks = contrib // STEP

    width = min(256, ny)

    def columns(at, carry):
        lanes = pl.ds(pl.multiple_of(at * width, width), width)
        small, big = column_factors(oy + at * width, col_ref[0], blocks, width)
        taper = window_ref[:, lanes] * b_scale
        small = (small[0] * taper, small[1] * taper)
        for a in range(blocks):
            c, s = turned(*big, a, *small)
            lo = a * STEP
            b_scr[lo : lo + STEP, lanes] = c.astype(jnp.bfloat16)
            b_scr[contrib + lo : contrib + lo + STEP, lanes] = (-s).astype(jnp.bfloat16)
        return carry

    lax.fori_loop(0, ny // width, columns, 0)
    load.wait()

    v = wrapped(ox + band_at * nx + iota((STEP, nx), 1))
    small_c, small_s = unit_circle(iota((STEP, nx), 0), v)
    small = (small_c * a_scale, small_s * a_scale)
    for s_at in range(per):

        def store(lo, c, s):
            a_scr[s_at, 0, lo : lo + STEP, :] = c
            a_scr[s_at, 1, lo : lo + STEP, :] = s

        row_table(rows_ref[sub_at * per + s_at], v, small, blocks, store)
    t = nt(b_scr[...], facet_scr[...])
    k = kern_ref[...]
    tr = nn(k, t[:contrib].astype(jnp.bfloat16)).astype(jnp.bfloat16)
    ti = nn(k, t[contrib:].astype(jnp.bfloat16)).astype(jnp.bfloat16)
    t_scr[0, :contrib, :] = tr
    t_scr[0, contrib:, :] = ti
    t_scr[1, :contrib, :] = -ti
    t_scr[1, contrib:, :] = tr
    for s_at in range(per):
        part = nt(t_scr[0], a_scr[s_at, 0]) + nt(t_scr[1], a_scr[s_at, 1])
        part_ref[0, s_at] = part[:contrib].astype(jnp.bfloat16)
        part_ref[1, s_at] = part[contrib:].astype(jnp.bfloat16)


def tables_kernel(
    where_ref, offs_ref, rows_ref, col_ref, kern_ref, after_ref, a_ref, d_ref, a_scr, d_scr,
    *, bands, subs, per, contrib, a_scale, d_scale,
):
    del after_ref
    facet_at, band_at, sub_at = place(where_ref, bands, subs)
    ox = offs_ref[0, facet_at]
    oy = offs_ref[1, facet_at]
    nx, ny = a_ref.shape[3], d_ref.shape[1]
    blocks = contrib // STEP
    k = kern_ref[...]
    v = wrapped(ox + band_at * nx + iota((STEP, nx), 1))
    small_c, small_s = unit_circle(iota((STEP, nx), 0), v)
    small = (small_c * a_scale, small_s * a_scale)
    for s_at in range(per):

        def store(lo, c, s):
            a_scr[s_at % 2, 0, lo : lo + STEP, :] = c
            a_scr[s_at % 2, 1, lo : lo + STEP, :] = s

        row_table(rows_ref[sub_at * per + s_at], v, small, blocks, store)
        for c_at in range(2):
            a_ref[s_at, c_at] = nn(k, a_scr[s_at % 2, c_at]).astype(jnp.bfloat16)
    width = min(256, ny)

    def columns(at, carry):
        lanes = pl.ds(pl.multiple_of(at * width, width), width)
        small, big = column_factors(oy + at * width, col_ref[0], blocks, width)
        small = (small[0] * d_scale, small[1] * d_scale)
        for a in range(blocks):
            c, s = turned(*big, a, *small)
            lo = a * STEP
            d_scr[0, lo : lo + STEP, :] = c.astype(jnp.bfloat16)
            d_scr[1, lo : lo + STEP, :] = (-s).astype(jnp.bfloat16)
        d_ref[:contrib, lanes] = nn(k, d_scr[0]).astype(jnp.bfloat16)
        d_ref[contrib:, lanes] = nn(k, d_scr[1]).astype(jnp.bfloat16)
        return carry

    lax.fori_loop(0, ny // width, columns, 0)


def middle_kernel(
    where_ref, lines_ref, a_hbm, kern_ref, counts_ref, e_ref, a_scr, w_scr, sems,
    *, subs, per, contrib, tile,
):
    loads = [pltpu.make_async_copy(a_hbm.at[s], a_scr.at[s], sems.at[s]) for s in range(per)]
    for load in loads:
        load.start()
    sub_at = where_ref[0] % subs
    tiles = contrib // tile
    k = kern_ref[...]
    spread = (iota((tiles, contrib), 1) // tile == iota((tiles, contrib), 0)).astype(jnp.bfloat16)
    for s in range(per):
        count = nn(counts_ref[sub_at * per + s], spread)
        weight = (count / (count + 4.0))[:, None, :]
        wr, wi = (
            (weight * nt(lines_ref[c, s], k).reshape(tiles, tile, contrib)).reshape(contrib, contrib)
            for c in range(2)
        )
        w_scr[s, 0, :contrib, :] = wr.astype(jnp.bfloat16)
        w_scr[s, 0, contrib:, :] = wi.astype(jnp.bfloat16)
        w_scr[s, 1, :contrib, :] = wi.astype(jnp.bfloat16)
        w_scr[s, 1, contrib:, :] = (-wr).astype(jnp.bfloat16)
    total = None
    for s in range(per):
        loads[s].wait()
        here = nn(w_scr[s, 0], a_scr[s, 0]) + nn(w_scr[s, 1], a_scr[s, 1])
        total = here if total is None else total + here
    e_ref[...] = total.T.astype(jnp.bfloat16)


def backward_kernel(mine_ref, other_ref, d_ref, window_ref, out_hbm, out_scr, sems, *, chunks):
    cols = out_scr.shape[1] // chunks
    e = (mine_ref[...].astype(jnp.float32) + other_ref[...].astype(jnp.float32)).astype(jnp.bfloat16)
    sends = []
    for j in range(chunks):
        here = slice(j * cols, (j + 1) * cols)
        image = nn(e, d_ref[:, here])
        out_scr[:, here] = (window_ref[:, here] * image).astype(jnp.bfloat16)
        send = pltpu.make_async_copy(
            out_scr.at[:, pl.ds(j * cols, cols)], out_hbm.at[:, pl.ds(j * cols, cols)], sems.at[j]
        )
        send.start()
        sends.append(send)
    for send in sends:
        send.wait()


def exchanged(x, axes):
    return lax.all_to_all(x, axes, 0, 0, tiled=True)


def summed(x):
    return jnp.sum(x.astype(jnp.float32), axis=0).astype(jnp.bfloat16)


def distant(x):
    return pltpu.with_memory_space_constraint(x, pltpu.HBM)


def near(x):
    return pltpu.with_memory_space_constraint(x, pltpu.VMEM)


def body(facets, window, facet_offsets, row_offsets, column_offset, kernel, tile_counts):
    bands, subs = lax.axis_size("zl"), lax.axis_size("core")
    plane, depth = lax.axis_size(PLANE), lax.axis_size(DEPTH)
    facet_count = plane * depth // bands
    nx, ny = facets.shape
    contrib = kernel.shape[0]
    per = row_offsets.shape[0] // subs
    tile = contrib // tile_counts.shape[1]
    a_scale = 1.0 / math.sqrt(ny * facet_count)
    b_scale = 1.0 / math.sqrt(ny)
    back_scale = 1.0 / math.sqrt(row_offsets.shape[0] * contrib)
    d_scale = back_scale / a_scale / math.sqrt(contrib)
    here = lax.axis_index(ROWS + ("core",)).astype(jnp.int32).reshape(1)
    taper = window.reshape(1, ny)
    offsets = facet_offsets.T
    smem = pl.BlockSpec(memory_space=pltpu.SMEM)
    vmem = pl.BlockSpec(memory_space=pltpu.VMEM)
    anywhere = pl.BlockSpec(memory_space=pl.ANY)
    far = pl.BlockSpec(memory_space=pltpu.HBM)

    part = pl.pallas_call(
        lambda *refs: forward_kernel(
            *refs, bands=bands, subs=subs, per=per, contrib=contrib, a_scale=a_scale, b_scale=b_scale,
        ),
        out_shape=pltpu.VMEM((2, per, contrib, contrib), jnp.bfloat16),
        in_specs=[smem, smem, smem, smem, vmem, vmem, far],
        out_specs=vmem,
        scratch_shapes=[
            pltpu.VMEM((nx, ny), jnp.bfloat16),
            pltpu.VMEM((2 * contrib, ny), jnp.bfloat16),
            pltpu.VMEM((2, 2 * contrib, nx), jnp.bfloat16),
            pltpu.VMEM((per, 2, contrib, nx), jnp.bfloat16),
            pltpu.SemaphoreType.DMA(()),
        ],
        compiler_params=pltpu.CompilerParams(vmem_limit_bytes=28 * 2**20),
        name="forward",
    )(here, distant(offsets), distant(row_offsets), column_offset, distant(taper), distant(kernel), distant(facets))

    lines = 2 * per * contrib
    mine = summed(exchanged(part.reshape(plane, lines // plane, contrib), PLANE))
    a_table, d_table = pl.pallas_call(
        lambda *refs: tables_kernel(
            *refs, bands=bands, subs=subs, per=per, contrib=contrib, a_scale=a_scale, d_scale=d_scale,
        ),
        out_shape=(
            pltpu.HBM((per, 2, contrib, nx), jnp.bfloat16),
            pltpu.VMEM((2 * contrib, ny), jnp.bfloat16),
        ),
        in_specs=[smem, smem, smem, smem, vmem, anywhere],
        out_specs=(vmem, vmem),
        scratch_shapes=[
            pltpu.VMEM((2, 2, contrib, nx), jnp.bfloat16),
            pltpu.VMEM((2, contrib, min(256, ny)), jnp.bfloat16),
        ],
        cost_estimate=pl.CostEstimate(flops=6_000_000_000, transcendentals=0, bytes_accessed=4_000_000),
        compiler_params=pltpu.CompilerParams(vmem_limit_bytes=20 * 2**20),
        name="tables",
    )(here, offsets, row_offsets, column_offset, kernel, mine)
    mine = summed(exchanged(mine.reshape(depth, lines // plane // depth, contrib), DEPTH))
    mine = exchanged(jnp.broadcast_to(mine, (depth, *mine.shape)), DEPTH)
    mine = mine.reshape(lines // plane, contrib)
    grid = exchanged(jnp.broadcast_to(mine, (plane, *mine.shape)), PLANE)
    grid = grid.reshape(2, per, contrib, contrib)

    counts = jnp.swapaxes(tile_counts, 1, 2).astype(jnp.bfloat16)
    e_part = pl.pallas_call(
        lambda *refs: middle_kernel(*refs, subs=subs, per=per, contrib=contrib, tile=tile),
        out_shape=pltpu.VMEM((nx, 2 * contrib), jnp.bfloat16),
        in_specs=[smem, vmem, far, vmem, vmem],
        out_specs=vmem,
        scratch_shapes=[
            pltpu.VMEM((per, 2, contrib, nx), jnp.bfloat16),
            pltpu.VMEM((per, 2, 2 * contrib, contrib), jnp.bfloat16),
            pltpu.SemaphoreType.DMA((per,)),
        ],
        compiler_params=pltpu.CompilerParams(vmem_limit_bytes=28 * 2**20),
        name="middle",
    )(here, near(grid), distant(a_table), kernel, counts)

    other = lax.ppermute(e_part, "core", [(i, (i + 1) % subs) for i in range(subs)])
    chunks = 4
    return pl.pallas_call(
        lambda *refs: backward_kernel(*refs, chunks=chunks),
        out_shape=jax.ShapeDtypeStruct((nx, ny), jnp.bfloat16),
        in_specs=[vmem, vmem, vmem, vmem],
        out_specs=far,
        scratch_shapes=[pltpu.VMEM((nx, ny), jnp.bfloat16), pltpu.SemaphoreType.DMA((chunks,))],
        compiler_params=pltpu.CompilerParams(vmem_limit_bytes=28 * 2**20),
        name="backward",
    )(near(e_part), near(other), near(d_table), taper)


def solution(mesh):
    fine = Mesh(np.asarray(mesh.devices).reshape(4, 4, 4, 4, 2), ROWS + ("core",))
    rows = P(ROWS, None)
    return jax.shard_map(
        body,
        mesh=fine,
        in_specs=(rows, P(), P(), P(), P(), P(), P()),
        out_specs=rows,
        check_vma=False,
    )
```

```python
import math

import jax
import jax.numpy as jnp
import numpy as np
from jax import lax
from jax.experimental import pallas as pl
from jax.experimental.pallas import tpu as pltpu
from jax.sharding import Mesh
from jax.sharding import PartitionSpec as P

IMAGE = 49152
STEP = 16
PLANE = ("y", "x")
DEPTH = ("zh", "zl")
ROWS = ("y", "zh", "x", "zl")


def wrapped(value):
    return jnp.where(value >= IMAGE, value - IMAGE, value)


def unit_circle(first, second):
    whole = first * second
    upper = lax.shift_right_logical(whole, jnp.int32(14))
    thirds = jnp.floor((upper.astype(jnp.float32) + 0.5) * (1.0 / 3.0)).astype(jnp.int32)
    reduced = (whole & 16383) + ((upper - 3 * thirds) << 14)
    turns = reduced.astype(jnp.float32)
    quarter = jnp.floor(turns * (4.0 / IMAGE) + 0.5)
    angle = (turns - quarter * (IMAGE / 4)) * (2.0 * math.pi / IMAGE)
    q = quarter.astype(jnp.int32)
    z = angle * angle
    sine = angle + angle * z * (
        -1.6666654611e-1 + z * (8.3321608736e-3 + z * -1.9515295891e-4)
    )
    cosine = 1.0 - 0.5 * z + z * z * (
        4.166664568298827e-2 + z * (-1.388731625493765e-3 + z * 2.443315711809948e-5)
    )
    odd = (q & 1) == 1
    c = jnp.where(odd, sine, cosine)
    s = jnp.where(odd, cosine, sine)
    c = jnp.where(((q + 1) & 2) == 2, -c, c)
    s = jnp.where((q & 2) == 2, -s, s)
    return c, s


def iota(shape, dim):
    return lax.broadcasted_iota(jnp.int32, shape, dim)


def nt(a, b):
    return lax.dot_general(a, b, (((1,), (1,)), ((), ())), preferred_element_type=jnp.float32)


def nn(a, b):
    return lax.dot_general(a, b, (((1,), (0,)), ((), ())), preferred_element_type=jnp.float32)


def turned(big_c, big_s, a, small_c, small_s):
    gc, gs = big_c[a : a + 1], big_s[a : a + 1]
    return gc * small_c - gs * small_s, gc * small_s + gs * small_c


def place(where_ref, bands, subs):
    me = where_ref[0]
    return me // (bands * subs), (me // subs) % bands, me % subs


def column_factors(oy, start, blocks, ny):
    v = wrapped(oy + iota((STEP, ny), 1))
    return unit_circle(iota((STEP, ny), 0), v), unit_circle(
        wrapped(start + STEP * iota((blocks, ny), 0)), v
    )


def row_table(start, v, small, blocks, store):
    big_c, big_s = unit_circle(wrapped(start + STEP * iota((blocks, v.shape[1]), 0)), v)
    for a in range(blocks):
        c, s = turned(big_c, big_s, a, *small)
        store(a * STEP, c.astype(jnp.bfloat16), (-s).astype(jnp.bfloat16))


def forward_kernel(
    where_ref, col_ref, offs_hbm, rows_hbm, window_hbm, kern_hbm, facet_hbm,
    part_ref, offs_ref, rows_ref, window_ref, kern_ref, facet_scr, b_scr, t_scr, a_scr, sems,
    *, bands, subs, per, contrib, a_scale, b_scale,
):
    loads = [
        pltpu.make_async_copy(source, target, sems.at[i])
        for i, (source, target) in enumerate((
            (offs_hbm, offs_ref), (rows_hbm, rows_ref), (window_hbm, window_ref),
            (kern_hbm, kern_ref), (facet_hbm, facet_scr),
        ))
    ]
    for load in loads:
        load.start()
    for load in loads[:3]:
        load.wait()
    facet_at, band_at, sub_at = place(where_ref, bands, subs)
    ox = offs_ref[0, facet_at]
    oy = offs_ref[1, facet_at]
    nx, ny = facet_scr.shape
    blocks = contrib // STEP

    width = min(256, ny)

    def columns(at, carry):
        lanes = pl.ds(pl.multiple_of(at * width, width), width)
        small, big = column_factors(oy + at * width, col_ref[0], blocks, width)
        taper = window_ref[:, lanes] * b_scale
        small = (small[0] * taper, small[1] * taper)
        for a in range(blocks):
            c, s = turned(*big, a, *small)
            lo = a * STEP
            b_scr[lo : lo + STEP, lanes] = c.astype(jnp.bfloat16)
            b_scr[contrib + lo : contrib + lo + STEP, lanes] = (-s).astype(jnp.bfloat16)
        return carry

    lax.fori_loop(0, ny // width, columns, 0)
    for load in loads[3:]:
        load.wait()

    v = wrapped(ox + band_at * nx + iota((STEP, nx), 1))
    small_c, small_s = unit_circle(iota((STEP, nx), 0), v)
    small = (small_c * a_scale, small_s * a_scale)
    for s_at in range(per):

        def store(lo, c, s):
            a_scr[s_at, 0, lo : lo + STEP, :] = c
            a_scr[s_at, 1, lo : lo + STEP, :] = s

        row_table(rows_ref[sub_at * per + s_at], v, small, blocks, store)
    t = nt(b_scr[...], facet_scr[...])
    k = kern_ref[...]
    tr = nn(k, t[:contrib].astype(jnp.bfloat16)).astype(jnp.bfloat16)
    ti = nn(k, t[contrib:].astype(jnp.bfloat16)).astype(jnp.bfloat16)
    t_scr[0, :contrib, :] = tr
    t_scr[0, contrib:, :] = ti
    t_scr[1, :contrib, :] = -ti
    t_scr[1, contrib:, :] = tr
    for s_at in range(per):
        part = nt(t_scr[0], a_scr[s_at, 0]) + nt(t_scr[1], a_scr[s_at, 1])
        part_ref[0, s_at] = part[:contrib].astype(jnp.bfloat16)
        part_ref[1, s_at] = part[contrib:].astype(jnp.bfloat16)


def tables_kernel(
    where_ref, offs_ref, rows_ref, col_ref, kern_ref, after_ref, a_ref, d_ref, a_scr, d_scr,
    *, bands, subs, per, contrib, a_scale, d_scale,
):
    del after_ref
    facet_at, band_at, sub_at = place(where_ref, bands, subs)
    ox = offs_ref[0, facet_at]
    oy = offs_ref[1, facet_at]
    nx, ny = a_ref.shape[3], d_ref.shape[1]
    blocks = contrib // STEP
    k = kern_ref[...]
    v = wrapped(ox + band_at * nx + iota((STEP, nx), 1))
    small_c, small_s = unit_circle(iota((STEP, nx), 0), v)
    small = (small_c * a_scale, small_s * a_scale)
    for s_at in range(per):

        def store(lo, c, s):
            a_scr[s_at % 2, 0, lo : lo + STEP, :] = c
            a_scr[s_at % 2, 1, lo : lo + STEP, :] = s

        row_table(rows_ref[sub_at * per + s_at], v, small, blocks, store)
        for c_at in range(2):
            a_ref[s_at, c_at] = nn(k, a_scr[s_at % 2, c_at]).astype(jnp.bfloat16)
    width = min(256, ny)

    def columns(at, carry):
        lanes = pl.ds(pl.multiple_of(at * width, width), width)
        small, big = column_factors(oy + at * width, col_ref[0], blocks, width)
        small = (small[0] * d_scale, small[1] * d_scale)
        for a in range(blocks):
            c, s = turned(*big, a, *small)
            lo = a * STEP
            d_scr[0, lo : lo + STEP, :] = c.astype(jnp.bfloat16)
            d_scr[1, lo : lo + STEP, :] = (-s).astype(jnp.bfloat16)
        d_ref[:contrib, lanes] = nn(k, d_scr[0]).astype(jnp.bfloat16)
        d_ref[contrib:, lanes] = nn(k, d_scr[1]).astype(jnp.bfloat16)
        return carry

    lax.fori_loop(0, ny // width, columns, 0)


def middle_kernel(
    where_ref, lines_ref, a_hbm, kern_ref, counts_ref, e_ref, a_scr, w_scr, sems,
    *, subs, per, contrib, tile,
):
    loads = [pltpu.make_async_copy(a_hbm.at[s], a_scr.at[s], sems.at[s]) for s in range(per)]
    for load in loads:
        load.start()
    sub_at = where_ref[0] % subs
    tiles = contrib // tile
    k = kern_ref[...]
    spread = (iota((tiles, contrib), 1) // tile == iota((tiles, contrib), 0)).astype(jnp.bfloat16)
    for s in range(per):
        count = nn(counts_ref[sub_at * per + s], spread)
        weight = (count / (count + 4.0))[:, None, :]
        wr, wi = (
            (weight * nt(lines_ref[c, s], k).reshape(tiles, tile, contrib)).reshape(contrib, contrib)
            for c in range(2)
        )
        w_scr[s, 0, :contrib, :] = wr.astype(jnp.bfloat16)
        w_scr[s, 0, contrib:, :] = wi.astype(jnp.bfloat16)
        w_scr[s, 1, :contrib, :] = wi.astype(jnp.bfloat16)
        w_scr[s, 1, contrib:, :] = (-wr).astype(jnp.bfloat16)
    total = None
    for s in range(per):
        loads[s].wait()
        here = nn(w_scr[s, 0], a_scr[s, 0]) + nn(w_scr[s, 1], a_scr[s, 1])
        total = here if total is None else total + here
    e_ref[...] = total.T.astype(jnp.bfloat16)


def backward_kernel(mine_ref, other_ref, d_ref, window_ref, out_hbm, out_scr, sems, *, chunks):
    cols = out_scr.shape[1] // chunks
    e = (mine_ref[...].astype(jnp.float32) + other_ref[...].astype(jnp.float32)).astype(jnp.bfloat16)
    sends = []
    for j in range(chunks):
        here = slice(j * cols, (j + 1) * cols)
        image = nn(e, d_ref[:, here])
        out_scr[:, here] = (window_ref[:, here] * image).astype(jnp.bfloat16)
        send = pltpu.make_async_copy(
            out_scr.at[:, pl.ds(j * cols, cols)], out_hbm.at[:, pl.ds(j * cols, cols)], sems.at[j]
        )
        send.start()
        sends.append(send)
    for send in sends:
        send.wait()


def exchanged(x, axes):
    return lax.all_to_all(x, axes, 0, 0, tiled=True)


def summed(x):
    return jnp.sum(x.astype(jnp.float32), axis=0).astype(jnp.bfloat16)


def distant(x):
    return pltpu.with_memory_space_constraint(x, pltpu.HBM)


def near(x):
    return pltpu.with_memory_space_constraint(x, pltpu.VMEM)


def body(facets, window, facet_offsets, row_offsets, column_offset, kernel, tile_counts):
    bands, subs = lax.axis_size("zl"), lax.axis_size("core")
    plane, depth = lax.axis_size(PLANE), lax.axis_size(DEPTH)
    facet_count = plane * depth // bands
    nx, ny = facets.shape
    contrib = kernel.shape[0]
    per = row_offsets.shape[0] // subs
    tile = contrib // tile_counts.shape[1]
    a_scale = 1.0 / math.sqrt(ny * facet_count)
    b_scale = 1.0 / math.sqrt(ny)
    back_scale = 1.0 / math.sqrt(row_offsets.shape[0] * contrib)
    d_scale = back_scale / a_scale / math.sqrt(contrib)
    here = lax.axis_index(ROWS + ("core",)).astype(jnp.int32).reshape(1)
    taper = window.reshape(1, ny)
    offsets = facet_offsets.T
    smem = pl.BlockSpec(memory_space=pltpu.SMEM)
    vmem = pl.BlockSpec(memory_space=pltpu.VMEM)
    anywhere = pl.BlockSpec(memory_space=pl.ANY)
    far = pl.BlockSpec(memory_space=pltpu.HBM)

    part = pl.pallas_call(
        lambda *refs: forward_kernel(
            *refs, bands=bands, subs=subs, per=per, contrib=contrib, a_scale=a_scale, b_scale=b_scale,
        ),
        out_shape=pltpu.VMEM((2, per, contrib, contrib), jnp.bfloat16),
        in_specs=[smem, smem, far, far, far, far, far],
        out_specs=vmem,
        scratch_shapes=[
            pltpu.SMEM(offsets.shape, jnp.int32),
            pltpu.SMEM(row_offsets.shape, jnp.int32),
            pltpu.VMEM(taper.shape, jnp.float32),
            pltpu.VMEM(kernel.shape, jnp.bfloat16),
            pltpu.VMEM((nx, ny), jnp.bfloat16),
            pltpu.VMEM((2 * contrib, ny), jnp.bfloat16),
            pltpu.VMEM((2, 2 * contrib, nx), jnp.bfloat16),
            pltpu.VMEM((per, 2, contrib, nx), jnp.bfloat16),
            pltpu.SemaphoreType.DMA((5,)),
        ],
        compiler_params=pltpu.CompilerParams(vmem_limit_bytes=28 * 2**20),
        name="forward",
    )(here, column_offset, distant(offsets), distant(row_offsets), distant(taper), distant(kernel), distant(facets))

    lines = 2 * per * contrib
    mine = summed(exchanged(part.reshape(plane, lines // plane, contrib), PLANE))
    a_table, d_table = pl.pallas_call(
        lambda *refs: tables_kernel(
            *refs, bands=bands, subs=subs, per=per, contrib=contrib, a_scale=a_scale, d_scale=d_scale,
        ),
        out_shape=(
            pltpu.HBM((per, 2, contrib, nx), jnp.bfloat16),
            pltpu.VMEM((2 * contrib, ny), jnp.bfloat16),
        ),
        in_specs=[smem, smem, smem, smem, vmem, anywhere],
        out_specs=(vmem, vmem),
        scratch_shapes=[
            pltpu.VMEM((2, 2, contrib, nx), jnp.bfloat16),
            pltpu.VMEM((2, contrib, min(256, ny)), jnp.bfloat16),
        ],
        cost_estimate=pl.CostEstimate(flops=6_000_000_000, transcendentals=0, bytes_accessed=4_000_000),
        compiler_params=pltpu.CompilerParams(vmem_limit_bytes=20 * 2**20),
        name="tables",
    )(here, offsets, row_offsets, column_offset, kernel, mine)
    mine = summed(exchanged(mine.reshape(depth, lines // plane // depth, contrib), DEPTH))
    mine = exchanged(jnp.broadcast_to(mine, (depth, *mine.shape)), DEPTH)
    mine = mine.reshape(lines // plane, contrib)
    grid = exchanged(jnp.broadcast_to(mine, (plane, *mine.shape)), PLANE)
    grid = grid.reshape(2, per, contrib, contrib)

    counts = jnp.swapaxes(tile_counts, 1, 2).astype(jnp.bfloat16)
    e_part = pl.pallas_call(
        lambda *refs: middle_kernel(*refs, subs=subs, per=per, contrib=contrib, tile=tile),
        out_shape=pltpu.VMEM((nx, 2 * contrib), jnp.bfloat16),
        in_specs=[smem, vmem, far, vmem, vmem],
        out_specs=vmem,
        scratch_shapes=[
            pltpu.VMEM((per, 2, contrib, nx), jnp.bfloat16),
            pltpu.VMEM((per, 2, 2 * contrib, contrib), jnp.bfloat16),
            pltpu.SemaphoreType.DMA((per,)),
        ],
        compiler_params=pltpu.CompilerParams(vmem_limit_bytes=28 * 2**20),
        name="middle",
    )(here, near(grid), distant(a_table), kernel, counts)

    other = lax.ppermute(e_part, "core", [(i, (i + 1) % subs) for i in range(subs)])
    chunks = 8
    return pl.pallas_call(
        lambda *refs: backward_kernel(*refs, chunks=chunks),
        out_shape=jax.ShapeDtypeStruct((nx, ny), jnp.bfloat16),
        in_specs=[vmem, vmem, vmem, vmem],
        out_specs=far,
        scratch_shapes=[pltpu.VMEM((nx, ny), jnp.bfloat16), pltpu.SemaphoreType.DMA((chunks,))],
        compiler_params=pltpu.CompilerParams(vmem_limit_bytes=28 * 2**20),
        name="backward",
    )(near(e_part), near(other), near(d_table), taper)


def solution(mesh):
    fine = Mesh(np.asarray(mesh.devices).reshape(4, 4, 4, 4, 2), ROWS + ("core",))
    rows = P(ROWS, None)
    return jax.shard_map(
        body,
        mesh=fine,
        in_specs=(rows, P(), P(), P(), P(), P(), P()),
        out_specs=rows,
        check_vma=False,
    )
```

```python
import math

import jax
import jax.numpy as jnp
import numpy as np
from jax import lax
from jax.experimental import pallas as pl
from jax.experimental.pallas import tpu as pltpu
from jax.sharding import Mesh
from jax.sharding import PartitionSpec as P

IMAGE = 49152
STEP = 16
PLANE = ("y", "x")
DEPTH = ("zh", "zl")
ROWS = ("y", "zh", "x", "zl")


def wrapped(value):
    return jnp.where(value >= IMAGE, value - IMAGE, value)


def unit_circle(first, second):
    whole = first * second
    upper = lax.shift_right_logical(whole, jnp.int32(14))
    thirds = jnp.floor((upper.astype(jnp.float32) + 0.5) * (1.0 / 3.0)).astype(jnp.int32)
    reduced = (whole & 16383) + ((upper - 3 * thirds) << 14)
    turns = reduced.astype(jnp.float32)
    quarter = jnp.floor(turns * (4.0 / IMAGE) + 0.5)
    angle = (turns - quarter * (IMAGE / 4)) * (2.0 * math.pi / IMAGE)
    q = quarter.astype(jnp.int32)
    z = angle * angle
    sine = angle + angle * z * (
        -1.6666654611e-1 + z * (8.3321608736e-3 + z * -1.9515295891e-4)
    )
    cosine = 1.0 - 0.5 * z + z * z * (
        4.166664568298827e-2 + z * (-1.388731625493765e-3 + z * 2.443315711809948e-5)
    )
    odd = (q & 1) == 1
    c = jnp.where(odd, sine, cosine)
    s = jnp.where(odd, cosine, sine)
    c = jnp.where(((q + 1) & 2) == 2, -c, c)
    s = jnp.where((q & 2) == 2, -s, s)
    return c, s


def iota(shape, dim):
    return lax.broadcasted_iota(jnp.int32, shape, dim)


def nt(a, b):
    return lax.dot_general(a, b, (((1,), (1,)), ((), ())), preferred_element_type=jnp.float32)


def nn(a, b):
    return lax.dot_general(a, b, (((1,), (0,)), ((), ())), preferred_element_type=jnp.float32)


def turned(big_c, big_s, a, small_c, small_s):
    gc, gs = big_c[a : a + 1], big_s[a : a + 1]
    return gc * small_c - gs * small_s, gc * small_s + gs * small_c


def place(where_ref, bands, subs):
    me = where_ref[0]
    return me // (bands * subs), (me // subs) % bands, me % subs


def column_factors(oy, start, blocks, ny):
    v = wrapped(oy + iota((STEP, ny), 1))
    return unit_circle(iota((STEP, ny), 0), v), unit_circle(
        wrapped(start + STEP * iota((blocks, ny), 0)), v
    )


def row_table(start, v, small, blocks, store):
    big_c, big_s = unit_circle(wrapped(start + STEP * iota((blocks, v.shape[1]), 0)), v)
    for a in range(blocks):
        c, s = turned(big_c, big_s, a, *small)
        store(a * STEP, c.astype(jnp.bfloat16), (-s).astype(jnp.bfloat16))


def forward_kernel(
    where_ref, col_ref, offs_hbm, rows_hbm, window_hbm, kern_hbm, facet_hbm,
    part_ref, offs_ref, rows_ref, window_ref, kern_ref, facet_scr, b_scr, t_scr, a_scr, sems,
    *, bands, subs, per, contrib, a_scale, b_scale,
):
    loads = [
        pltpu.make_async_copy(source, target, sems.at[i])
        for i, (source, target) in enumerate((
            (offs_hbm, offs_ref), (rows_hbm, rows_ref), (window_hbm, window_ref),
            (kern_hbm, kern_ref), (facet_hbm, facet_scr),
        ))
    ]
    for load in loads:
        load.start()
    for load in loads[:3]:
        load.wait()
    facet_at, band_at, sub_at = place(where_ref, bands, subs)
    ox = offs_ref[0, facet_at]
    oy = offs_ref[1, facet_at]
    nx, ny = facet_scr.shape
    blocks = contrib // STEP

    width = min(512, ny)

    def columns(at, carry):
        lanes = pl.ds(pl.multiple_of(at * width, width), width)
        small, big = column_factors(oy + at * width, col_ref[0], blocks, width)
        taper = window_ref[:, lanes] * b_scale
        small = (small[0] * taper, small[1] * taper)
        for a in range(blocks):
            c, s = turned(*big, a, *small)
            lo = a * STEP
            b_scr[lo : lo + STEP, lanes] = c.astype(jnp.bfloat16)
            b_scr[contrib + lo : contrib + lo + STEP, lanes] = (-s).astype(jnp.bfloat16)
        return carry

    lax.fori_loop(0, ny // width, columns, 0)
    for load in loads[3:]:
        load.wait()

    v = wrapped(ox + band_at * nx + iota((STEP, nx), 1))
    small_c, small_s = unit_circle(iota((STEP, nx), 0), v)
    small = (small_c * a_scale, small_s * a_scale)
    for s_at in range(per):

        def store(lo, c, s):
            a_scr[s_at, 0, lo : lo + STEP, :] = c
            a_scr[s_at, 1, lo : lo + STEP, :] = s

        row_table(rows_ref[sub_at * per + s_at], v, small, blocks, store)
    t = nt(b_scr[...], facet_scr[...])
    k = kern_ref[...]
    tr = nn(k, t[:contrib].astype(jnp.bfloat16)).astype(jnp.bfloat16)
    ti = nn(k, t[contrib:].astype(jnp.bfloat16)).astype(jnp.bfloat16)
    t_scr[0, :contrib, :] = tr
    t_scr[0, contrib:, :] = ti
    t_scr[1, :contrib, :] = -ti
    t_scr[1, contrib:, :] = tr
    for s_at in range(per):
        part = nt(t_scr[0], a_scr[s_at, 0]) + nt(t_scr[1], a_scr[s_at, 1])
        part_ref[0, s_at] = part[:contrib].astype(jnp.bfloat16)
        part_ref[1, s_at] = part[contrib:].astype(jnp.bfloat16)


def tables_kernel(
    where_ref, offs_ref, rows_ref, col_ref, kern_ref, after_ref, a_ref, d_ref, a_scr, d_scr,
    *, bands, subs, per, contrib, a_scale, d_scale,
):
    del after_ref
    facet_at, band_at, sub_at = place(where_ref, bands, subs)
    ox = offs_ref[0, facet_at]
    oy = offs_ref[1, facet_at]
    nx, ny = a_ref.shape[3], d_ref.shape[1]
    blocks = contrib // STEP
    k = kern_ref[...]
    v = wrapped(ox + band_at * nx + iota((STEP, nx), 1))
    small_c, small_s = unit_circle(iota((STEP, nx), 0), v)
    small = (small_c * a_scale, small_s * a_scale)
    for s_at in range(per):

        def store(lo, c, s):
            a_scr[s_at % 2, 0, lo : lo + STEP, :] = c
            a_scr[s_at % 2, 1, lo : lo + STEP, :] = s

        row_table(rows_ref[sub_at * per + s_at], v, small, blocks, store)
        for c_at in range(2):
            a_ref[s_at, c_at] = nn(k, a_scr[s_at % 2, c_at]).astype(jnp.bfloat16)
    width = min(256, ny)

    def columns(at, carry):
        lanes = pl.ds(pl.multiple_of(at * width, width), width)
        small, big = column_factors(oy + at * width, col_ref[0], blocks, width)
        small = (small[0] * d_scale, small[1] * d_scale)
        for a in range(blocks):
            c, s = turned(*big, a, *small)
            lo = a * STEP
            d_scr[0, lo : lo + STEP, :] = c.astype(jnp.bfloat16)
            d_scr[1, lo : lo + STEP, :] = (-s).astype(jnp.bfloat16)
        d_ref[:contrib, lanes] = nn(k, d_scr[0]).astype(jnp.bfloat16)
        d_ref[contrib:, lanes] = nn(k, d_scr[1]).astype(jnp.bfloat16)
        return carry

    lax.fori_loop(0, ny // width, columns, 0)


def middle_kernel(
    where_ref, lines_ref, a_ref, d_hbm, kern_ref, counts_ref, e_ref, d_ref, w_scr, sem,
    *, subs, per, contrib, tile,
):
    bring = pltpu.make_async_copy(d_hbm, d_ref, sem)
    bring.start()
    sub_at = where_ref[0] % subs
    tiles = contrib // tile
    k = kern_ref[...]
    spread = (iota((tiles, contrib), 1) // tile == iota((tiles, contrib), 0)).astype(jnp.bfloat16)
    for s in range(per):
        count = nn(counts_ref[sub_at * per + s], spread)
        weight = (count / (count + 4.0))[:, None, :]
        wr, wi = (
            (weight * nt(lines_ref[c, s], k).reshape(tiles, tile, contrib)).reshape(contrib, contrib)
            for c in range(2)
        )
        w_scr[s, 0, :contrib, :] = wr.astype(jnp.bfloat16)
        w_scr[s, 0, contrib:, :] = wi.astype(jnp.bfloat16)
        w_scr[s, 1, :contrib, :] = wi.astype(jnp.bfloat16)
        w_scr[s, 1, contrib:, :] = (-wr).astype(jnp.bfloat16)
    total = None
    for s in range(per):
        here = nn(w_scr[s, 0], a_ref[s, 0]) + nn(w_scr[s, 1], a_ref[s, 1])
        total = here if total is None else total + here
    e_ref[...] = total.T.astype(jnp.bfloat16)
    bring.wait()


def backward_kernel(mine_ref, other_ref, d_ref, window_ref, out_hbm, out_scr, sems, *, chunks):
    cols = out_scr.shape[1] // chunks
    e = (mine_ref[...].astype(jnp.float32) + other_ref[...].astype(jnp.float32)).astype(jnp.bfloat16)
    sends = []
    for j in range(chunks):
        here = slice(j * cols, (j + 1) * cols)
        image = nn(e, d_ref[:, here])
        out_scr[:, here] = (window_ref[:, here] * image).astype(jnp.bfloat16)
        send = pltpu.make_async_copy(
            out_scr.at[:, pl.ds(j * cols, cols)], out_hbm.at[:, pl.ds(j * cols, cols)], sems.at[j]
        )
        send.start()
        sends.append(send)
    for send in sends:
        send.wait()


def exchanged(x, axes):
    return lax.all_to_all(x, axes, 0, 0, tiled=True)


def summed(x):
    return jnp.sum(x.astype(jnp.float32), axis=0).astype(jnp.bfloat16)


def distant(x):
    return pltpu.with_memory_space_constraint(x, pltpu.HBM)


def near(x):
    return pltpu.with_memory_space_constraint(x, pltpu.VMEM)


def body(facets, window, facet_offsets, row_offsets, column_offset, kernel, tile_counts):
    bands, subs = lax.axis_size("zl"), lax.axis_size("core")
    plane, depth = lax.axis_size(PLANE), lax.axis_size(DEPTH)
    facet_count = plane * depth // bands
    nx, ny = facets.shape
    contrib = kernel.shape[0]
    per = row_offsets.shape[0] // subs
    tile = contrib // tile_counts.shape[1]
    a_scale = 1.0 / math.sqrt(ny * facet_count)
    b_scale = 1.0 / math.sqrt(ny)
    back_scale = 1.0 / math.sqrt(row_offsets.shape[0] * contrib)
    d_scale = back_scale / a_scale / math.sqrt(contrib)
    here = lax.axis_index(ROWS + ("core",)).astype(jnp.int32).reshape(1)
    taper = window.reshape(1, ny)
    offsets = facet_offsets.T
    smem = pl.BlockSpec(memory_space=pltpu.SMEM)
    vmem = pl.BlockSpec(memory_space=pltpu.VMEM)
    anywhere = pl.BlockSpec(memory_space=pl.ANY)
    far = pl.BlockSpec(memory_space=pltpu.HBM)

    part = pl.pallas_call(
        lambda *refs: forward_kernel(
            *refs, bands=bands, subs=subs, per=per, contrib=contrib, a_scale=a_scale, b_scale=b_scale,
        ),
        out_shape=pltpu.VMEM((2, per, contrib, contrib), jnp.bfloat16),
        in_specs=[smem, smem, far, far, far, far, far],
        out_specs=vmem,
        scratch_shapes=[
            pltpu.SMEM(offsets.shape, jnp.int32),
            pltpu.SMEM(row_offsets.shape, jnp.int32),
            pltpu.VMEM(taper.shape, jnp.float32),
            pltpu.VMEM(kernel.shape, jnp.bfloat16),
            pltpu.VMEM((nx, ny), jnp.bfloat16),
            pltpu.VMEM((2 * contrib, ny), jnp.bfloat16),
            pltpu.VMEM((2, 2 * contrib, nx), jnp.bfloat16),
            pltpu.VMEM((per, 2, contrib, nx), jnp.bfloat16),
            pltpu.SemaphoreType.DMA((5,)),
        ],
        compiler_params=pltpu.CompilerParams(vmem_limit_bytes=28 * 2**20),
        name="forward",
    )(here, column_offset, distant(offsets), distant(row_offsets), distant(taper), distant(kernel), distant(facets))

    lines = 2 * per * contrib
    mine = summed(exchanged(part.reshape(plane, lines // plane, contrib), PLANE))
    a_table, d_table = pl.pallas_call(
        lambda *refs: tables_kernel(
            *refs, bands=bands, subs=subs, per=per, contrib=contrib, a_scale=a_scale, d_scale=d_scale,
        ),
        out_shape=(
            pltpu.VMEM((per, 2, contrib, nx), jnp.bfloat16),
            pltpu.HBM((2 * contrib, ny), jnp.bfloat16),
        ),
        in_specs=[smem, smem, smem, smem, vmem, anywhere],
        out_specs=(vmem, vmem),
        scratch_shapes=[
            pltpu.VMEM((2, 2, contrib, nx), jnp.bfloat16),
            pltpu.VMEM((2, contrib, min(256, ny)), jnp.bfloat16),
        ],
        cost_estimate=pl.CostEstimate(flops=6_000_000_000, transcendentals=0, bytes_accessed=4_000_000),
        compiler_params=pltpu.CompilerParams(vmem_limit_bytes=20 * 2**20),
        name="tables",
    )(here, offsets, row_offsets, column_offset, kernel, mine)
    mine = summed(exchanged(mine.reshape(depth, lines // plane // depth, contrib), DEPTH))
    mine = exchanged(jnp.broadcast_to(mine, (depth, *mine.shape)), DEPTH)
    mine = mine.reshape(lines // plane, contrib)
    grid = exchanged(jnp.broadcast_to(mine, (plane, *mine.shape)), PLANE)
    grid = grid.reshape(2, per, contrib, contrib)

    counts = jnp.swapaxes(tile_counts, 1, 2).astype(jnp.bfloat16)
    e_part, d_table = pl.pallas_call(
        lambda *refs: middle_kernel(*refs, subs=subs, per=per, contrib=contrib, tile=tile),
        out_shape=(
            pltpu.VMEM((nx, 2 * contrib), jnp.bfloat16),
            pltpu.VMEM((2 * contrib, ny), jnp.bfloat16),
        ),
        in_specs=[smem, vmem, vmem, far, vmem, vmem],
        out_specs=(vmem, vmem),
        scratch_shapes=[
            pltpu.VMEM((per, 2, 2 * contrib, contrib), jnp.bfloat16),
            pltpu.SemaphoreType.DMA(()),
        ],
        compiler_params=pltpu.CompilerParams(vmem_limit_bytes=28 * 2**20),
        name="middle",
    )(here, near(grid), near(a_table), distant(d_table), kernel, counts)

    other = lax.ppermute(e_part, "core", [(i, (i + 1) % subs) for i in range(subs)])
    chunks = 4
    return pl.pallas_call(
        lambda *refs: backward_kernel(*refs, chunks=chunks),
        out_shape=jax.ShapeDtypeStruct((nx, ny), jnp.bfloat16),
        in_specs=[vmem, vmem, vmem, vmem],
        out_specs=far,
        scratch_shapes=[pltpu.VMEM((nx, ny), jnp.bfloat16), pltpu.SemaphoreType.DMA((chunks,))],
        compiler_params=pltpu.CompilerParams(vmem_limit_bytes=28 * 2**20),
        name="backward",
    )(near(e_part), near(other), near(d_table), taper)


def solution(mesh):
    fine = Mesh(np.asarray(mesh.devices).reshape(4, 4, 4, 4, 2), ROWS + ("core",))
    rows = P(ROWS, None)
    return jax.shard_map(
        body,
        mesh=fine,
        in_specs=(rows, P(), P(), P(), P(), P(), P()),
        out_specs=rows,
        check_vma=False,
    )
```
